128 devices in a mesh: dp: 8 (over y, x_lo), tp: 16 (over z, x_hi, core).
Axes of the slice: x: 4 (x_hi: 2, x_lo: 2; x = x_hi * 2 + x_lo), y: 4, z: 4, core: 2. Of those that a mesh axis runs over, the one named last changes fastest.
Arguments:
- gradients: bfloat16 [8, 4, 3072, 768], P('dp', None, 'tp'), may hold values from -6 to 6, as said below
- right_factor: float32 [4, 768, 8], replicated, may hold values from -6 to 6
- weights_before: float32 [4, 3072, 768], P(None, 'tp', 'dp'), may hold values from -0.21875 to 0.21875
- momentum: float32 [4, 3072, 768], P(None, 'tp', 'dp'), may hold values from -0.3125 to 0.3125
Outputs:
- new_weights: float32 [4, 3072, 768], P(None, 'tp', 'dp')
- new_basis: float32 [4, 768, 8], replicated
- new_momentum: float32 [4, 3072, 768], P(None, 'tp', 'dp')
The draws below stay inside these ranges and needn't reach their ends.
Inputs may be any that keep to these rules, and one draw needn't show every extreme that they name: gradients holds numbers from -6 to 6.
All inputs are finite; a program needn't handle non-finite values.
Results may differ from the reference program's by a relative error of at most 0.0003.
Values sent between devices are 32-bit elements.
A program may use at most 64 MiB of HBM per device.

```python
import jax
import jax.numpy as jnp
from jax import lax

WIDTH = 768
INNER = 3072
RANK = 8
LAYERS = 4
REPLICAS = 8
N_TP = 16


def draw_gradients(key, part):
    keys = jax.random.split(key, 5)
    level = jnp.exp(jax.random.uniform(keys[4], (1, LAYERS, N_TP, 1, RANK), jnp.float32, -1.3, 1.3))
    left = jax.random.normal(keys[0], (1, LAYERS, N_TP, INNER // N_TP, RANK), jnp.float32) * level
    left = left.reshape(1, LAYERS, INNER, RANK)
    right = jax.random.normal(keys[1], (1, LAYERS, RANK, WIDTH), jnp.float32)
    strength = jax.random.normal(keys[2], (REPLICAS, LAYERS, 1, RANK), jnp.float32)
    noise = jax.random.normal(keys[3], (REPLICAS, LAYERS, INNER, WIDTH), jnp.float32)
    low = jnp.einsum('alir,lrw->aliw', left * strength, right[0])
    values = low * RANK ** (-0.5) + 0.5 * noise
    return jnp.clip(values, -6.0, 6.0).astype(jnp.bfloat16)


def levels(own_key, shape, pieces, smallest, high):
    gain, own = 1.0, jax.random.fold_in(own_key, 6)
    for position, shards_of in pieces:
        steps = jnp.exp(jax.random.uniform(jax.random.fold_in(own, position), (shards_of,), jnp.float32, smallest / len(pieces), high / len(pieces)))
        gain = gain * jnp.repeat(steps, shape[position] // shards_of).reshape([-1 if axis == position else 1 for axis in range(len(shape))])
    return gain


def gaussian(stream_key, shape, spread, bound, cuts=(), held_as=jnp.bfloat16):
    gain = levels(stream_key, shape, cuts, -0.22, 0.18) if cuts else 1.0
    values = jax.random.normal(stream_key, shape, jnp.float32) * spread * gain
    return jnp.minimum(jnp.maximum(values, -bound), bound).astype(held_as)


def setup_inputs(seed: int = 0) -> dict:
    splits = jax.random.split(jax.random.key(seed), 5)
    return {
        "gradients": draw_gradients(jax.random.fold_in(splits[4], 71), 0),
        "right_factor": gaussian(splits[1], (LAYERS, WIDTH, RANK), 1.0, 6.0, (), jnp.float32),
        "weights_before": gaussian(splits[2], (LAYERS, INNER, WIDTH), WIDTH ** -0.5, 0.21875, ((1, 16), (2, 8)), jnp.float32),
        "momentum": gaussian(splits[3], (LAYERS, INNER, WIDTH), 0.05, 0.3125, ((1, 16), (2, 8)), jnp.float32),
    }


def reference(gradients, right_factor, weights_before, momentum):
    small_basis = right_factor.astype(jnp.bfloat16)
    small_basis = lax.optimization_barrier(small_basis)
    left = jnp.einsum('aliw,lwr->lir', gradients.astype(jnp.float32), small_basis.astype(jnp.float32))
    gram = jnp.einsum('lir,lis->lrs', left, left, precision=lax.Precision.HIGHEST)
    gram = gram + 0.001 * lax.optimization_barrier(jnp.mean(jnp.diagonal(gram, axis1=1, axis2=2), axis=1))[:, None, None] * jnp.eye(RANK, dtype=jnp.float32)
    small_left = lax.optimization_barrier(left.astype(jnp.bfloat16))
    right = jnp.einsum('aliw,lir->lwr', gradients.astype(jnp.float32), small_left.astype(jnp.float32))
    root = jnp.linalg.cholesky(gram)
    half = lax.linalg.triangular_solve(root, jnp.swapaxes(right, 1, 2), left_side=True, lower=True)
    mixed = lax.linalg.triangular_solve(root, half, left_side=True, lower=True, transpose_a=True)
    change = jnp.einsum('lir,lrw->liw', left, mixed, precision=lax.Precision.HIGHEST) / REPLICAS
    new_momentum = 0.9 * momentum + change
    new_weights = weights_before - 0.02 * new_momentum
    new_basis = right * lax.rsqrt(lax.optimization_barrier(jnp.mean(right * right, axis=(1, 2), keepdims=True)) + 1e-12)
    return (new_weights, new_basis, new_momentum)
```

```python
import functools

import jax
import jax.numpy as jnp
from jax import lax
from jax.experimental import pallas as pl
from jax.experimental.pallas import tpu as pltpu
from jax.sharding import PartitionSpec as P

RANK = 8
LANES = 128
MESH = pl.DeviceIdType.MESH
F32 = jnp.float32
BF16 = jnp.bfloat16


def remote(src, dst, send_sem, recv_sem, dp, tp):
    return pltpu.make_async_remote_copy(
        src_ref=src,
        dst_ref=dst,
        send_sem=send_sem,
        recv_sem=recv_sem,
        device_id=(dp, tp),
        device_id_type=MESH,
    )


def take_bytes(ref, sem):
    pltpu.make_async_copy(ref, ref, sem).wait()


def split3(value):
    high = value.astype(BF16).astype(F32)
    rest = value - high
    middle = rest.astype(BF16).astype(F32)
    return high, middle, rest - middle


def kernel(
    n_dp,
    n_far,
    grads_hbm,
    factor_ref,
    weights_hbm,
    momentum_hbm,
    new_weights_ref,
    new_basis_ref,
    new_momentum_ref,
    grads,
    weights,
    momentum,
    lefts,
    pieces,
    parts,
    sums,
    whole,
    turned,
    load_sems,
    send_sems,
    recv_sems,
):
    layers, rows, width = grads.shape
    cols = width // n_dp
    half = layers // 2
    dp = lax.axis_index("dp")
    tp = lax.axis_index("tp")
    core = lax.rem(tp, 2)
    far = tp // 2
    group = dp * 2 + core

    def dp_peer(k):
        return lax.rem(dp + k, n_dp)

    def far_peer(k):
        return lax.rem(far + k, n_far)

    barrier = pltpu.get_barrier_semaphore()

    def greet(to_dp, to_tp):
        pl.semaphore_signal(barrier, inc=1, device_id=(to_dp, to_tp), device_id_type=MESH)

    other = far * 2 + (1 - core)
    for k in range(1, n_far):
        greet(dp, far_peer(k) * 2 + core)
    for k in range(1, n_dp):
        greet(dp_peer(k), tp)
        greet(dp_peer(k), other)
    greet(dp, other)

    loads = [
        pltpu.make_async_copy(grads_hbm.at[l], grads.at[l], load_sems.at[l]) for l in range(layers)
    ]
    late = [
        pltpu.make_async_copy(weights_hbm, weights, load_sems.at[layers]),
        pltpu.make_async_copy(momentum_hbm, momentum, load_sems.at[layers + 1]),
    ]
    for load in loads + late:
        load.start()

    left_parts = []
    for l in range(layers):
        loads[l].wait()
        left_parts.append(
            lax.dot_general(
                factor_ref[l].astype(BF16),
                grads[l],
                (((1,), (1,)), ((), ())),
                preferred_element_type=F32,
            )
        )
    for l in range(layers):
        lefts[dp, l] = left_parts[l][:, :LANES]
    for h in range(half):
        lefts[dp, layers + h] = jnp.concatenate(
            [left_parts[2 * h][:, LANES:], left_parts[2 * h + 1][:, LANES:]], axis=1
        )

    pl.semaphore_wait(barrier, n_far - 1 + 2 * n_dp - 1)

    copies_a = [
        remote(lefts.at[dp], lefts.at[dp], send_sems.at[0], recv_sems.at[0], dp_peer(k), tp)
        for k in range(1, n_dp)
    ]
    for copy in copies_a:
        copy.start()
    take_bytes(lefts.at[pl.ds(0, n_dp - 1)], recv_sems.at[0])

    total = lefts[0]
    for k in range(1, n_dp):
        total = total + lefts[k]
    rest = rows - LANES
    left = []
    for l in range(layers):
        tail = total[layers + l // 2][:, (l % 2) * rest : (l % 2 + 1) * rest]
        left.append(jnp.concatenate([total[l], tail], axis=1))

    for l in range(layers):
        right = jnp.dot(left[l].astype(BF16), grads[l], preferred_element_type=F32)
        gram = lax.dot_general(
            left[l],
            left[l],
            (((1,), (1,)), ((), ())),
            precision=lax.Precision.HIGHEST,
            preferred_element_type=F32,
        ) * (1.0 / n_dp)
        spare = jnp.concatenate(
            [gram, jnp.zeros((RANK, LANES - cols - RANK), F32)], axis=1
        )
        for d in range(n_dp):
            pieces[d * 2 + l // half, l % half] = jnp.concatenate(
                [right[:, d * cols : (d + 1) * cols], spare], axis=1
            )

    copies_1 = []
    for k in range(n_dp):
        for side in range(2):
            if k == 0 and side == 0:
                continue
            to_core = core if side == 0 else 1 - core
            to_dp = dp_peer(k)
            copies_1.append(
                remote(
                    pieces.at[to_dp * 2 + to_core],
                    parts.at[group],
                    send_sems.at[1],
                    recv_sems.at[1],
                    to_dp,
                    far * 2 + to_core,
                )
            )
    for copy in copies_1:
        copy.start()
    parts[group] = pieces[group]

    for l in range(layers):
        high, middle, low = split3(left[l])
        turned[l] = jnp.concatenate(
            [high, high, middle, high, middle, low], axis=0
        ).T.astype(BF16)

    n_group = 2 * n_dp
    take_bytes(parts.at[pl.ds(0, n_group - 1)], recv_sems.at[1])
    own = parts[0]
    for k in range(1, n_group):
        own = own + parts[k]
    sums[far] = own

    copies_2 = [
        remote(
            sums.at[far], sums.at[far], send_sems.at[2], recv_sems.at[2], dp, far_peer(k) * 2 + core
        )
        for k in range(1, n_far)
    ]
    for copy in copies_2:
        copy.start()
    take_bytes(sums.at[pl.ds(0, n_far - 1)], recv_sems.at[2])
    own = sums[0]
    for k in range(1, n_far):
        own = own + sums[k]
    whole[group] = own

    near = remote(
        whole.at[group], whole.at[group], send_sems.at[3], recv_sems.at[3], dp, other
    )
    near.start()
    copies_3 = []
    for k in range(1, n_dp):
        for to_tp in (tp, other):
            copies_3.append(
                remote(
                    whole.at[group],
                    whole.at[group],
                    send_sems.at[4],
                    recv_sems.at[4],
                    dp_peer(k),
                    to_tp,
                )
            )
    for copy in copies_3:
        copy.start()

    near.wait_recv()
    tile = jnp.concatenate([whole[dp * 2], whole[dp * 2 + 1]], axis=0)
    row = lax.broadcasted_iota(jnp.int32, tile.shape, 1)
    lane = lax.broadcasted_iota(jnp.int32, tile.shape, 2)
    diagonal = lane == row + cols
    trace = jnp.sum(jnp.where(diagonal, tile, 0.0), axis=(1, 2), keepdims=True)
    tile = tile + jnp.where(diagonal, trace * (0.001 / RANK), 0.0)
    for k in range(RANK):
        pivot_row = tile[:, k : k + 1, :] / tile[:, k : k + 1, cols + k : cols + k + 1]
        column = tile[:, :, cols + k : cols + k + 1]
        tile = jnp.where(row == k, pivot_row, tile - column * pivot_row)
    mixed = tile * (1.0 / n_dp)

    for load in late:
        load.wait()
    for l in range(layers):
        high, middle, low = split3(mixed[l])
        stack = jnp.concatenate([high, middle, high, low, middle, high], axis=0).astype(BF16)
        change = jnp.dot(turned[l], stack, preferred_element_type=F32)[:, :cols]
        moved = 0.9 * momentum[l] + change
        new_momentum_ref[l] = moved
        new_weights_ref[l] = weights[l] - 0.02 * moved

    take_bytes(whole.at[pl.ds(0, n_group - 2)], recv_sems.at[4])
    for l in range(layers):
        right = jnp.concatenate(
            [whole[d * 2 + l // half, l % half][:, :cols] for d in range(n_dp)], axis=1
        )
        mean = jnp.sum(right * right, axis=(0, 1), keepdims=True) * (1.0 / (RANK * width))
        new_basis_ref[l] = right * lax.rsqrt(mean + 1e-12)

    take_bytes(lefts.at[pl.ds(0, n_dp - 1)], send_sems.at[0])
    take_bytes(parts.at[pl.ds(0, n_group - 1)], send_sems.at[1])
    take_bytes(sums.at[pl.ds(0, n_far - 1)], send_sems.at[2])
    near.wait_send()
    take_bytes(whole.at[pl.ds(0, n_group - 2)], send_sems.at[4])


def solution(mesh):
    n_dp = mesh.shape["dp"]
    n_far = mesh.shape["tp"] // 2

    def step(gradients, right_factor, weights_before, momentum):
        grads = gradients[0]
        factor = jnp.swapaxes(right_factor, 1, 2)
        layers, rows, width = grads.shape
        half = layers // 2
        block = weights_before.shape
        vmem = pl.BlockSpec(memory_space=pltpu.VMEM)
        hbm = pl.BlockSpec(memory_space=pl.ANY)
        tile = (half, RANK, LANES)
        new_weights, new_basis, new_momentum = pl.pallas_call(
            functools.partial(kernel, n_dp, n_far),
            out_shape=(
                jax.ShapeDtypeStruct(block, F32),
                jax.ShapeDtypeStruct(factor.shape, F32),
                jax.ShapeDtypeStruct(block, F32),
            ),
            in_specs=[hbm, vmem, hbm, hbm],
            out_specs=(vmem, vmem, vmem),
            scratch_shapes=[
                pltpu.VMEM(grads.shape, BF16),
                pltpu.VMEM(block, F32),
                pltpu.VMEM(block, F32),
                pltpu.VMEM((n_dp, layers + half, RANK, LANES), F32),
                pltpu.VMEM((2 * n_dp,) + tile, F32),
                pltpu.VMEM((2 * n_dp,) + tile, F32),
                pltpu.VMEM((n_far,) + tile, F32),
                pltpu.VMEM((2 * n_dp,) + tile, F32),
                pltpu.VMEM((layers, rows, 6 * RANK), BF16),
                pltpu.SemaphoreType.DMA((layers + 2,)),
                pltpu.SemaphoreType.DMA((5,)),
                pltpu.SemaphoreType.DMA((5,)),
            ],
            compiler_params=pltpu.CompilerParams(collective_id=0, has_side_effects=True),
        )(grads, factor, weights_before, momentum)
        return new_weights, jnp.swapaxes(new_basis, 1, 2), new_momentum

    return jax.shard_map(
        step,
        mesh=mesh,
        in_specs=(P("dp", None, "tp", None), P(), P(None, "tp", "dp"), P(None, "tp", "dp")),
        out_specs=(P(None, "tp", "dp"), P(), P(None, "tp", "dp")),
        check_vma=False,
    )
```

```python
import functools

import jax
import jax.numpy as jnp
from jax import lax
from jax.experimental import pallas as pl
from jax.experimental.pallas import tpu as pltpu
from jax.sharding import PartitionSpec as P

RANK = 8
LANES = 128
MESH = pl.DeviceIdType.MESH
F32 = jnp.float32
BF16 = jnp.bfloat16


def remote(src, dst, send_sem, recv_sem, dp, tp):
    return pltpu.make_async_remote_copy(
        src_ref=src,
        dst_ref=dst,
        send_sem=send_sem,
        recv_sem=recv_sem,
        device_id=(dp, tp),
        device_id_type=MESH,
    )


def take_bytes(ref, sem):
    pltpu.make_async_copy(ref, ref, sem).wait()


def farthest(ring, step):
    def hops(offset):
        return min(offset[0], ring - offset[0]) + step * offset[1]

    offsets = [(up, over) for up in range(ring) for over in range(2) if up or over]
    return sorted(offsets, key=hops, reverse=True)


def split3(value):
    high = value.astype(BF16).astype(F32)
    rest = value - high
    middle = rest.astype(BF16).astype(F32)
    return high, middle, rest - middle


def kernel(
    n_dp,
    n_far,
    grads_hbm,
    factor_hbm,
    weights_hbm,
    momentum_hbm,
    new_weights_ref,
    new_basis_ref,
    new_momentum_ref,
    grads,
    factor,
    weights,
    momentum,
    lefts,
    pieces,
    parts,
    sums,
    whole,
    turned,
    load_sems,
    send_sems,
    recv_sems,
):
    layers, rows, width = grads.shape
    cols = width // n_dp
    half = layers // 2
    dp = lax.axis_index("dp")
    tp = lax.axis_index("tp")
    core = lax.rem(tp, 2)
    far = tp // 2
    group = dp * 2 + core

    dp_peers = [
        lax.rem(dp // 2 + up, n_dp // 2) * 2 + lax.rem(dp + over, 2)
        for up, over in farthest(n_dp // 2, 1)
    ]
    far_peers = [
        lax.rem(far // 2 + up, n_far // 2) * 2 + lax.rem(far + over, 2)
        for up, over in farthest(n_far // 2, 2)
    ]

    barrier = pltpu.get_barrier_semaphore()

    def greet(to_dp, to_tp):
        pl.semaphore_signal(barrier, inc=1, device_id=(to_dp, to_tp), device_id_type=MESH)

    other = far * 2 + (1 - core)
    for peer in far_peers:
        greet(dp, peer * 2 + core)
    for peer in dp_peers:
        greet(peer, tp)
        greet(peer, other)
    greet(dp, other)

    loads = [
        pltpu.make_async_copy(grads_hbm.at[l], grads.at[l], load_sems.at[l]) for l in range(layers)
    ]
    late = [
        pltpu.make_async_copy(weights_hbm, weights, load_sems.at[layers]),
        pltpu.make_async_copy(momentum_hbm, momentum, load_sems.at[layers + 1]),
    ]
    first = pltpu.make_async_copy(factor_hbm, factor, load_sems.at[layers + 2])
    for load in [first] + loads + late:
        load.start()

    left_parts = []
    first.wait()
    for l in range(layers):
        loads[l].wait()
        left_parts.append(
            lax.dot_general(
                factor[l].astype(BF16),
                grads[l],
                (((1,), (1,)), ((), ())),
                preferred_element_type=F32,
            )
        )
    for l in range(layers):
        lefts[dp, l] = left_parts[l][:, :LANES]
    for h in range(half):
        lefts[dp, layers + h] = jnp.concatenate(
            [left_parts[2 * h][:, LANES:], left_parts[2 * h + 1][:, LANES:]], axis=1
        )

    pl.semaphore_wait(barrier, n_far - 1 + 2 * n_dp - 1)

    copies_a = [
        remote(lefts.at[dp], lefts.at[dp], send_sems.at[0], recv_sems.at[0], peer, tp)
        for peer in dp_peers
    ]
    for copy in copies_a:
        copy.start()
    take_bytes(lefts.at[pl.ds(0, n_dp - 1)], recv_sems.at[0])

    total = lefts[0]
    for k in range(1, n_dp):
        total = total + lefts[k]
    rest = rows - LANES
    left = []
    for l in range(layers):
        tail = total[layers + l // 2][:, (l % 2) * rest : (l % 2 + 1) * rest]
        left.append(jnp.concatenate([total[l], tail], axis=1))

    for l in range(layers):
        right = jnp.dot(left[l].astype(BF16), grads[l], preferred_element_type=F32)
        gram = lax.dot_general(
            left[l],
            left[l],
            (((1,), (1,)), ((), ())),
            precision=lax.Precision.HIGHEST,
            preferred_element_type=F32,
        ) * (1.0 / n_dp)
        spare = jnp.concatenate(
            [gram, jnp.zeros((RANK, LANES - cols - RANK), F32)], axis=1
        )
        for d in range(n_dp):
            pieces[d * 2 + l // half, l % half] = jnp.concatenate(
                [right[:, d * cols : (d + 1) * cols], spare], axis=1
            )

    copies_1 = []
    for to_dp in dp_peers + [dp]:
        for to_core in (core, 1 - core) if to_dp is not dp else (1 - core,):
            copies_1.append(
                remote(
                    pieces.at[to_dp * 2 + to_core],
                    parts.at[group],
                    send_sems.at[1],
                    recv_sems.at[1],
                    to_dp,
                    far * 2 + to_core,
                )
            )
    for copy in copies_1:
        copy.start()
    parts[group] = pieces[group]

    for l in range(layers):
        high, middle, low = split3(left[l])
        turned[l] = jnp.concatenate(
            [high, high, middle, high, middle, low], axis=0
        ).T.astype(BF16)

    n_group = 2 * n_dp
    take_bytes(parts.at[pl.ds(0, n_group - 1)], recv_sems.at[1])
    own = parts[0]
    for k in range(1, n_group):
        own = own + parts[k]
    sums[far] = own

    copies_2 = [
        remote(
            sums.at[far], sums.at[far], send_sems.at[2], recv_sems.at[2], dp, peer * 2 + core
        )
        for peer in far_peers
    ]
    for copy in copies_2:
        copy.start()
    take_bytes(sums.at[pl.ds(0, n_far - 1)], recv_sems.at[2])
    own = sums[0]
    for k in range(1, n_far):
        own = own + sums[k]
    whole[group] = own

    near = remote(
        whole.at[group], whole.at[group], send_sems.at[3], recv_sems.at[3], dp, other
    )
    near.start()
    copies_3 = []
    for peer in dp_peers:
        for to_tp in (tp, other):
            copies_3.append(
                remote(
                    whole.at[group],
                    whole.at[group],
                    send_sems.at[4],
                    recv_sems.at[4],
                    peer,
                    to_tp,
                )
            )
    for copy in copies_3:
        copy.start()

    near.wait_recv()
    tile = jnp.concatenate([whole[dp * 2], whole[dp * 2 + 1]], axis=0)
    row = lax.broadcasted_iota(jnp.int32, tile.shape, 1)
    lane = lax.broadcasted_iota(jnp.int32, tile.shape, 2)
    diagonal = lane == row + cols
    trace = jnp.sum(jnp.where(diagonal, tile, 0.0), axis=(1, 2), keepdims=True)
    tile = tile + jnp.where(diagonal, trace * (0.001 / RANK), 0.0)
    for k in range(RANK):
        pivot_row = tile[:, k : k + 1, :] / tile[:, k : k + 1, cols + k : cols + k + 1]
        column = tile[:, :, cols + k : cols + k + 1]
        tile = jnp.where(row == k, pivot_row, tile - column * pivot_row)
    mixed = tile * (1.0 / n_dp)

    for load in late:
        load.wait()
    for l in range(layers):
        high, middle, low = split3(mixed[l])
        stack = jnp.concatenate([high, middle, high, low, middle, high], axis=0).astype(BF16)
        change = jnp.dot(turned[l], stack, preferred_element_type=F32)[:, :cols]
        moved = 0.9 * momentum[l] + change
        new_momentum_ref[l] = moved
        new_weights_ref[l] = weights[l] - 0.02 * moved

    take_bytes(whole.at[pl.ds(0, n_group - 2)], recv_sems.at[4])
    for l in range(layers):
        right = jnp.concatenate(
            [whole[d * 2 + l // half, l % half][:, :cols] for d in range(n_dp)], axis=1
        )
        mean = jnp.sum(right * right, axis=(0, 1), keepdims=True) * (1.0 / (RANK * width))
        new_basis_ref[l] = right * lax.rsqrt(mean + 1e-12)

    take_bytes(lefts.at[pl.ds(0, n_dp - 1)], send_sems.at[0])
    take_bytes(parts.at[pl.ds(0, n_group - 1)], send_sems.at[1])
    take_bytes(sums.at[pl.ds(0, n_far - 1)], send_sems.at[2])
    near.wait_send()
    take_bytes(whole.at[pl.ds(0, n_group - 2)], send_sems.at[4])


def put_out(a_ref, b_ref, c_ref, a_hbm, b_hbm, c_hbm, sems):
    moves = [
        pltpu.make_async_copy(src, dst, sems.at[i])
        for i, (src, dst) in enumerate(((a_ref, a_hbm), (c_ref, c_hbm), (b_ref, b_hbm)))
    ]
    for move in moves:
        move.start()
    for move in moves:
        move.wait()


def solution(mesh):
    n_dp = mesh.shape["dp"]
    n_far = mesh.shape["tp"] // 2

    def step(gradients, right_factor, weights_before, momentum):
        grads = gradients[0]
        factor = jnp.swapaxes(right_factor, 1, 2)
        layers, rows, width = grads.shape
        half = layers // 2
        block = weights_before.shape
        vmem = pl.BlockSpec(memory_space=pltpu.VMEM)
        hbm = pl.BlockSpec(memory_space=pl.ANY)
        tile = (half, RANK, LANES)
        new_weights, new_basis, new_momentum = pl.pallas_call(
            functools.partial(kernel, n_dp, n_far),
            out_shape=(
                pltpu.VMEM(block, F32),
                pltpu.VMEM(factor.shape, F32),
                pltpu.VMEM(block, F32),
            ),
            in_specs=[hbm] * 4,
            out_specs=(vmem, vmem, vmem),
            scratch_shapes=[
                pltpu.VMEM(grads.shape, BF16),
                pltpu.VMEM(factor.shape, F32),
                pltpu.VMEM(block, F32),
                pltpu.VMEM(block, F32),
                pltpu.VMEM((n_dp, layers + half, RANK, LANES), F32),
                pltpu.VMEM((2 * n_dp,) + tile, F32),
                pltpu.VMEM((2 * n_dp,) + tile, F32),
                pltpu.VMEM((n_far,) + tile, F32),
                pltpu.VMEM((2 * n_dp,) + tile, F32),
                pltpu.VMEM((layers, rows, 6 * RANK), BF16),
                pltpu.SemaphoreType.DMA((layers + 3,)),
                pltpu.SemaphoreType.DMA((5,)),
                pltpu.SemaphoreType.DMA((5,)),
            ],
            compiler_params=pltpu.CompilerParams(collective_id=0, has_side_effects=True),
        )(grads, factor, weights_before, momentum)
        new_weights, new_basis, new_momentum = pl.pallas_call(
            put_out,
            out_shape=tuple(
                jax.ShapeDtypeStruct(v.shape, F32) for v in (new_weights, new_basis, new_momentum)
            ),
            in_specs=[vmem] * 3,
            out_specs=(hbm,) * 3,
            scratch_shapes=[pltpu.SemaphoreType.DMA((3,))],
            compiler_params=pltpu.CompilerParams(vmem_limit_bytes=1000000),
        )(new_weights, new_basis, new_momentum)
        return new_weights, jnp.swapaxes(new_basis, 1, 2), new_momentum

    return jax.shard_map(
        step,
        mesh=mesh,
        in_specs=(P("dp", None, "tp", None), P(), P(None, "tp", "dp"), P(None, "tp", "dp")),
        out_specs=(P(None, "tp", "dp"), P(), P(None, "tp", "dp")),
        check_vma=False,
    )
```
